32 devices in a mesh: shard: 4 (over z), rep: 8 (over y, x, core).
Axes of the slice: x: 2, y: 2, z: 4, core: 2. Of those that a mesh axis runs over, the one named last changes fastest.
Arguments:
- inputs: bfloat16 [16, 1024, 1088], P('rep', 'shard'), may hold values from -6 to 6
- segments: int32 [16, 1024], P('rep'), may hold values from 0 to 2, never falling along the last dimension, each value on 1 to 640 neighbouring positions
- cotangent: bfloat16 [16, 1024, 1088], P('rep', 'shard'), may hold values from -6 to 6
- ln_gain: bfloat16 [2, 1088], P(None, 'shard'), may hold values from 0.099609375 to 1.8984375
- ln_bias: bfloat16 [2, 1088], P(None, 'shard'), may hold values from -3 to 3
- w_qkv: bfloat16 [1088, 3264], P(None, 'shard'), may hold values from -0.1875 to 0.1875
- qv_bias: bfloat16 [1, 2176], P(None, 'shard'), may hold values from -0.29882812 to 0.29882812
- w_out: bfloat16 [1088, 1088], P(None, 'shard'), may hold values from -3 to 3
- out_bias: bfloat16 [2, 1088], P(None, 'shard'), may hold values from -2 to 2
- w_fc1: bfloat16 [1088, 4352], P(None, 'shard'), may hold values from -0.1875 to 0.1875
- fc1_bias: bfloat16 [1, 4352], P(None, 'shard'), may hold values from -3 to 3
- w_fc2: bfloat16 [4352, 1088], P(None, 'shard'), may hold values from -0.09375 to 0.09375
Outputs:
- output: bfloat16 [16, 1024, 1088], P('rep', 'shard')
- d_inputs: bfloat16 [16, 1024, 1088], P('rep', 'shard')
- g_ln_gain: float32 [2, 1088], P(None, 'shard')
- g_ln_bias: float32 [2, 1088], P(None, 'shard')
- g_w_qkv: float32 [1088, 3264], P(None, 'shard')
- g_qv_bias: float32 [1, 2176], P(None, 'shard')
- g_w_out: float32 [1088, 1088], P(None, 'shard')
- g_out_bias: float32 [2, 1088], P(None, 'shard')
- g_w_fc1: float32 [1088, 4352], P(None, 'shard')
- g_fc1_bias: float32 [1, 4352], P(None, 'shard')
- g_w_fc2: float32 [4352, 1088], P(None, 'shard')
The draws below stay inside these ranges and needn't reach their ends.
Inputs may be any that keep to these rules, and one draw needn't show every extreme that they name: `segments`: within a sequence the document numbers never fall; each of the three documents holds 1 to 640 tokens, and one holds exactly 640.
All inputs are finite; a program needn't handle non-finite values.
Results may differ from the reference program's by a relative error of at most 0.018.
Values may be sent and summed in bfloat16 or wider, within the bound.
A program may use at most 320 MiB of HBM per device.

```python
import math
import jax
import jax.numpy as jnp
import numpy as np
from jax import lax

D = 1088
HEADS = 17
HEAD_DIM = 64
FF = 4352
SEQ = 1024
GROUPS = 16


def levels(own_key, dims, split, smallest, largest):
    def one(axis_at, blocks):
        draws = jax.random.uniform(jax.random.fold_in(jax.random.fold_in(own_key, 6), axis_at), (blocks,), jnp.float32, smallest / len(split), largest / len(split))
        return jnp.repeat(jnp.exp(draws), dims[axis_at] // blocks).reshape((-1,) + (1,) * (len(dims) - axis_at - 1))

    level = one(*split[0])
    for cut in split[1:]:
        level = level * one(*cut)
    return level


def profile(number_of, total, most, slope):
    loads = [(1 << 20) // math.isqrt(standing ** slope) + 1 for standing in range(2, number_of + 1)]
    surplus, counts = total - most - (number_of - 1), [1] * (number_of - 1)
    while surplus > 0:
        movable = [i for i in range(number_of - 1) if counts[i] < most]
        whole, budget = sum([loads[i] for i in movable]), surplus
        for i in movable:
            more = min(most - counts[i], max(1, budget * loads[i] // whole), surplus)
            counts[i] = counts[i] + more
            surplus = surplus - more
    return np.array([most] + counts)


def uneven(rng, number_of, total, limit, lean):
    if number_of == 2:
        one = jax.random.randint(rng, (), max(1, total - limit), min(limit, total - 1) + 1)
        return jnp.stack([one, total - one])
    lengths = jnp.asarray(profile(number_of, total, limit, lean), jnp.int32)
    couples = (number_of - 1) // 2
    giver, taker = lengths[1:1 + 2 * couples:2], lengths[2:2 + 2 * couples:2]
    room = jnp.minimum(giver - 1, limit - taker)
    shifted = jax.random.randint(jax.random.fold_in(rng, 1), (couples,), 0, 1 << 20) % (room + 1)
    lengths = lengths.at[1:1 + 2 * couples:2].set(giver - shifted).at[2:2 + 2 * couples:2].set(taker + shifted)
    return lengths[jax.random.permutation(jax.random.fold_in(rng, 2), number_of)]


def bell_draw(rng, shape, width, reach, shards=(), kind=jnp.bfloat16):
    level = levels(rng, shape, shards, -0.22, 0.18) if shards else 1.0
    entries = jax.random.normal(rng, shape, jnp.float32) * width * level
    return jnp.minimum(jnp.maximum(entries, -reach), reach).astype(kind)


def setup_inputs(seed: int = 0) -> dict:
    seeds = jax.random.split(jax.random.key(seed), 13)
    inputs = bell_draw(seeds[0], (GROUPS, SEQ, D), 1.0, 6.0, ((0, 8), (1, 4)))
    segments = jax.vmap(lambda own: jnp.searchsorted(jnp.cumsum(uneven(own, 3, SEQ, 5 * SEQ // 8, 0)), jnp.arange(SEQ), side="right"))(jax.random.split(seeds[1], GROUPS)).reshape((GROUPS, SEQ)).astype(jnp.int32)
    cotangent = bell_draw(seeds[2], (GROUPS, SEQ, D), 1.0, 6.0, ((0, 8), (1, 4)))
    ln_gain = jnp.clip(1.0 + 0.18 * jax.random.normal(seeds[3], (2, D), jnp.float32), 0.099609375, 1.8984375).astype(jnp.bfloat16)
    ln_bias = bell_draw(seeds[4], (2, D), 0.5, 3.0, ((1, 4),))
    w_qkv = bell_draw(seeds[5], (D, 3 * D), D ** -0.5, 0.1875, ((1, 4),))
    qv_bias = bell_draw(seeds[6], (1, 2 * D), 0.05, 0.29882812, ((1, 4),))
    w_out = bell_draw(seeds[7], (D, D), (max(D // 256, 1)) ** -0.5, 3.0, ((1, 4),))
    out_bias = bell_draw(seeds[8], (2, D), 0.3, 2.0, ((1, 4),))
    w_fc1 = bell_draw(seeds[9], (D, FF), D ** -0.5, 0.1875, ((1, 4),))
    fc1_bias = bell_draw(seeds[10], (1, FF), 0.5, 3.0, ((1, 4),))
    w_fc2 = bell_draw(seeds[11], (FF, D), FF ** -0.5, 0.09375, ((1, 4),))
    return {"inputs": inputs, "segments": segments, "cotangent": cotangent, "ln_gain": ln_gain, "ln_bias": ln_bias, "w_qkv": w_qkv, "qv_bias": qv_bias, "w_out": w_out, "out_bias": out_bias, "w_fc1": w_fc1, "fc1_bias": fc1_bias, "w_fc2": w_fc2}


@jax.custom_vjp
def low(v):
    return lax.optimization_barrier(v.astype(jnp.bfloat16)).astype(jnp.float32)

@jax.custom_vjp
def low_back(v):
    return v

def low_keep(v):
    return (low(v), None)

def low_pass(kept, grad):
    return (grad,)

def back_keep(v):
    return (v, None)

def back_low(kept, grad):
    return (low(grad),)
low.defvjp(low_keep, low_pass)
low_back.defvjp(back_keep, back_low)

def matmul(left, right):
    return jnp.dot(left, right, precision=lax.Precision.HIGHEST)

def layer_norm(values, gain, bias):
    centered = values - lax.optimization_barrier(jnp.mean(values, -1, keepdims=True))
    factor = lax.rsqrt(lax.optimization_barrier(jnp.mean(centered * centered, -1, keepdims=True)) + 1e-05)
    return centered * factor * gain + bias

def layer(tokens, seg_row, ln_gain, ln_bias, w_qkv, qv_bias, w_out, out_bias, w_fc1, fc1_bias, w_fc2):
    length = tokens.shape[0]
    normed_one = low(layer_norm(tokens, ln_gain[0], ln_bias[0]))
    zero_block = jnp.zeros((D,), jnp.float32)
    bias_row = jnp.concatenate([qv_bias[0, :D], zero_block, qv_bias[0, D:]])
    qkv = low_back(low(matmul(normed_one, w_qkv) + bias_row))
    queries = qkv[:, :D].reshape(length, HEADS, HEAD_DIM)
    key_rows = qkv[:, D:2 * D].reshape(length, HEADS, HEAD_DIM)
    value_rows = qkv[:, 2 * D:].reshape(length, HEADS, HEAD_DIM)
    raw_scores = jnp.einsum('qhe,khe->hqk', queries, key_rows, precision=lax.Precision.HIGHEST) * HEAD_DIM ** (-0.5)
    raw_scores = low_back(raw_scores)
    positions = jnp.arange(length, dtype=jnp.int32)
    allowed = (positions[None, :] <= positions[:, None]) & (seg_row[None, :] == seg_row[:, None])
    attn_probs = jax.nn.softmax(jnp.where(allowed[None], raw_scores, -1e+30), axis=-1)
    attn_mixed = jnp.einsum('hqk,khe->qhe', low(attn_probs), value_rows, precision=lax.Precision.HIGHEST)
    attn_mixed = low_back(low(attn_mixed.reshape(length, D)))
    branch = low_back(matmul(attn_mixed, w_out) + out_bias[0])
    residual = tokens + branch
    normed_two = low(layer_norm(residual, ln_gain[1], ln_bias[1]))
    pre_act = low_back(matmul(normed_two, w_fc1) + fc1_bias[0])
    activated = low(jax.nn.gelu(pre_act, approximate=True))
    return residual + (matmul(activated, w_fc2) + out_bias[1])

def reference(inputs, segments, cotangent, ln_gain, ln_bias, w_qkv, qv_bias, w_out, out_bias, w_fc1, fc1_bias, w_fc2):
    params = tuple((item.astype(jnp.float32) for item in (ln_gain, ln_bias, w_qkv, qv_bias, w_out, out_bias, w_fc1, fc1_bias, w_fc2)))

    def sequence_step(grad_sums, block_item):
        tokens, seg_row, d_output = block_item

        def forward(tokens_in, *weights):
            return layer(tokens_in, seg_row, *weights)
        result, pull_back = jax.vjp(forward, tokens.astype(jnp.float32), *params)
        grad_list = pull_back(d_output.astype(jnp.float32))
        new_sums = tuple((old + new for old, new in zip(grad_sums, grad_list[1:])))
        return (new_sums, (result.astype(jnp.bfloat16), grad_list[0].astype(jnp.bfloat16)))
    zero_grads = tuple((jnp.zeros_like(item) for item in params))
    grad_sums, (outputs, d_inputs) = lax.scan(sequence_step, zero_grads, (inputs, segments, cotangent))
    return (outputs, d_inputs) + tuple(grad_sums)
```

```python
import jax
import jax.numpy as jnp
from jax import lax
from jax.experimental import pallas as pl
from jax.experimental.pallas import tpu as pltpu
from jax.sharding import PartitionSpec as P

HEADS = 17
HEAD_DIM = 64


def layer_norm(values, gain, bias):
    centered = values - jnp.mean(values, -1, keepdims=True)
    factor = lax.rsqrt(jnp.mean(centered * centered, -1, keepdims=True) + 1e-05)
    unit = centered * factor
    return (unit * gain + bias, unit, factor)


def norm_back(d_normed, unit, factor, gain):
    scaled = d_normed * gain
    return factor * (
        scaled
        - jnp.mean(scaled, -1, keepdims=True)
        - unit * jnp.mean(scaled * unit, -1, keepdims=True)
    )


def gelu_tanh(values):
    return jax.nn.gelu(values, approximate=True)


def block_scores(queries, key_block, query_pos, query_seg, pos_block, seg_block):
    raw_scores = jnp.einsum(
        "qhe,khe->hqk", queries, key_block, preferred_element_type=jnp.float32
    ) * HEAD_DIM ** (-0.5)
    allowed = (pos_block[None, :] <= query_pos[:, None]) & (
        seg_block[None, :] == query_seg[:, None]
    )
    return (raw_scores, allowed[None])


def split_blocks(key_all, value_all, seg_row):
    total_rows = key_all.shape[0]
    block_rows = min(512, total_rows)
    block_count = total_rows // block_rows
    key_blocks = key_all.reshape(block_count, block_rows, HEADS, HEAD_DIM)
    value_blocks = value_all.reshape(block_count, block_rows, HEADS, HEAD_DIM)
    pos_blocks = jnp.arange(total_rows, dtype=jnp.int32).reshape(block_count, block_rows)
    seg_blocks = seg_row.reshape(block_count, block_rows)
    return (key_blocks, value_blocks, pos_blocks, seg_blocks)


def attention_forward(queries, key_all, value_all, query_pos, query_seg, seg_row):
    key_blocks, value_blocks, pos_blocks, seg_blocks = split_blocks(key_all, value_all, seg_row)
    row_count = queries.shape[0]

    def gather_stats(state_pair, block_item):
        run_max, run_sum = state_pair
        key_block, pos_block, seg_block = block_item
        raw_scores, allowed = block_scores(
            queries, key_block, query_pos, query_seg, pos_block, seg_block
        )
        masked = jnp.where(allowed, raw_scores, -1e30)
        new_max = jnp.maximum(run_max, jnp.max(masked, -1))
        expo = jnp.where(allowed, jnp.exp(masked - new_max[..., None]), 0.0)
        run_sum = run_sum * jnp.exp(run_max - new_max) + jnp.sum(expo, -1)
        return ((new_max, run_sum), None)

    start_max = jnp.full((HEADS, row_count), -1e30, jnp.float32)
    start_sum = jnp.zeros((HEADS, row_count), jnp.float32)
    (run_max, run_sum), _ = lax.scan(
        gather_stats, (start_max, start_sum), (key_blocks, pos_blocks, seg_blocks)
    )
    log_total = run_max + jnp.log(run_sum)

    def gather_values(accum_out, block_item):
        key_block, value_block, pos_block, seg_block = block_item
        raw_scores, allowed = block_scores(
            queries, key_block, query_pos, query_seg, pos_block, seg_block
        )
        attn_probs = jnp.where(allowed, jnp.exp(raw_scores - log_total[..., None]), 0.0).astype(
            jnp.bfloat16
        )
        return (
            accum_out
            + jnp.einsum(
                "hqk,khe->qhe", attn_probs, value_block, preferred_element_type=jnp.float32
            ),
            None,
        )

    start_out = jnp.zeros((row_count, HEADS, HEAD_DIM), jnp.float32)
    accum_out, _ = lax.scan(
        gather_values, start_out, (key_blocks, value_blocks, pos_blocks, seg_blocks)
    )
    return (accum_out, log_total)


def attention_backward(
    queries, key_all, value_all, d_mixed, log_total, query_pos, query_seg, seg_row
):
    key_blocks, value_blocks, pos_blocks, seg_blocks = split_blocks(key_all, value_all, seg_row)
    row_count = queries.shape[0]
    scale = HEAD_DIM ** (-0.5)

    def probs_and_grads(block_item):
        key_block, value_block, pos_block, seg_block = block_item
        raw_scores, allowed = block_scores(
            queries, key_block, query_pos, query_seg, pos_block, seg_block
        )
        attn_probs = jnp.where(allowed, jnp.exp(raw_scores - log_total[..., None]), 0.0)
        d_probs = jnp.einsum(
            "qhe,khe->hqk", d_mixed, value_block, preferred_element_type=jnp.float32
        )
        return (attn_probs, d_probs)

    def gather_delta(row_delta, block_item):
        attn_probs, d_probs = probs_and_grads(block_item)
        return (row_delta + jnp.sum(attn_probs * d_probs, -1), None)

    blocks_all = (key_blocks, value_blocks, pos_blocks, seg_blocks)
    row_delta, _ = lax.scan(gather_delta, jnp.zeros((HEADS, row_count), jnp.float32), blocks_all)

    def gather_grads(d_queries, block_item):
        key_block = block_item[0]
        attn_probs, d_probs = probs_and_grads(block_item)
        d_scores = (attn_probs * (d_probs - row_delta[..., None])).astype(jnp.bfloat16)
        d_queries = (
            d_queries
            + jnp.einsum("hqk,khe->qhe", d_scores, key_block, preferred_element_type=jnp.float32)
            * scale
        )
        key_grad = (
            jnp.einsum("hqk,qhe->khe", d_scores, queries, preferred_element_type=jnp.float32)
            * scale
        )
        value_grad = jnp.einsum(
            "hqk,qhe->khe",
            attn_probs.astype(jnp.bfloat16),
            d_mixed,
            preferred_element_type=jnp.float32,
        )
        block_rows = key_block.shape[0]
        term = jnp.concatenate(
            [key_grad.reshape(block_rows, -1), value_grad.reshape(block_rows, -1)], 1
        )
        return (d_queries, term)

    start_grad = jnp.zeros((row_count, HEADS, HEAD_DIM), jnp.float32)
    d_queries, terms = lax.scan(gather_grads, start_grad, blocks_all)
    return (d_queries, terms.reshape(key_all.shape[0], -1))


def shards(
    inputs,
    segments,
    cotangent,
    ln_gain,
    ln_bias,
    w_qkv,
    qv_bias,
    w_out,
    out_bias,
    w_fc1,
    fc1_bias,
    w_fc2,
):
    row_count = inputs.shape[1]
    features = inputs.shape[2]
    shard_index = lax.axis_index("shard")
    query_pos = shard_index * row_count + jnp.arange(row_count, dtype=jnp.int32)
    gathered = (
        lax.all_gather(ln_gain, "shard", axis=1, tiled=True),
        lax.all_gather(ln_bias, "shard", axis=1, tiled=True),
        lax.all_gather(w_qkv, "shard", axis=1, tiled=True),
        lax.all_gather(qv_bias, "shard", axis=1, tiled=True),
        lax.all_gather(w_out, "shard", axis=1, tiled=True),
        lax.all_gather(out_bias, "shard", axis=1, tiled=True),
        lax.all_gather(w_fc1, "shard", axis=1, tiled=True),
        lax.all_gather(fc1_bias, "shard", axis=1, tiled=True),
        lax.all_gather(w_fc2, "shard", axis=1, tiled=True),
    )
    gain_rows = gathered[0].astype(jnp.float32)
    bias_rows = gathered[1].astype(jnp.float32)
    qv_row = gathered[3].astype(jnp.float32)
    out_rows = gathered[5].astype(jnp.float32)
    fc1_row = gathered[7].astype(jnp.float32)
    bias_full = jnp.concatenate(
        [qv_row[0, :features], jnp.zeros((features,), jnp.float32), qv_row[0, features:]]
    )

    def forward_step(marker, item):
        token_bf, seg_row = item
        tokens = token_bf.astype(jnp.float32)
        query_seg = lax.dynamic_slice_in_dim(seg_row, shard_index * row_count, row_count)
        normed_f32, unit_one, factor_one = layer_norm(tokens, gain_rows[0], bias_rows[0])
        normed_one = normed_f32.astype(jnp.bfloat16)
        qkv = (
            jnp.dot(normed_one, gathered[2], preferred_element_type=jnp.float32) + bias_full
        ).astype(jnp.bfloat16)
        queries = qkv[:, :features].reshape(row_count, HEADS, HEAD_DIM)
        key_local = qkv[:, features : 2 * features]
        value_local = qkv[:, 2 * features :]
        key_all, value_all = (
            lax.all_gather(key_local, "shard", axis=0, tiled=True),
            lax.all_gather(value_local, "shard", axis=0, tiled=True),
        )
        attn_out, log_total = attention_forward(
            queries, key_all, value_all, query_pos, query_seg, seg_row
        )
        attn_mixed = attn_out.reshape(row_count, features).astype(jnp.bfloat16)
        branch = jnp.dot(attn_mixed, gathered[4], preferred_element_type=jnp.float32) + out_rows[0]
        residual = tokens + branch
        normed_f32, unit_two, factor_two = layer_norm(residual, gain_rows[1], bias_rows[1])
        normed_two = normed_f32.astype(jnp.bfloat16)
        pre_act = jnp.dot(normed_two, gathered[6], preferred_element_type=jnp.float32) + fc1_row[0]
        activated = gelu_tanh(pre_act).astype(jnp.bfloat16)
        output = residual + (
            jnp.dot(activated, gathered[8], preferred_element_type=jnp.float32) + out_rows[1]
        )
        saved = (
            normed_one,
            unit_one,
            factor_one,
            queries,
            key_local,
            value_local,
            log_total,
            attn_mixed,
            unit_two,
            factor_two,
            normed_two,
            pre_act,
        )
        return (marker, (output.astype(jnp.bfloat16), saved, ()))

    _, (outputs, saved_all, kept_all) = lax.scan(
        forward_step, jnp.zeros((), jnp.float32), (inputs, segments)
    )
    regathered = (
        lax.all_gather(ln_gain, "shard", axis=1, tiled=True),
        lax.all_gather(ln_bias, "shard", axis=1, tiled=True),
        lax.all_gather(w_qkv, "shard", axis=1, tiled=True),
        lax.all_gather(qv_bias, "shard", axis=1, tiled=True),
        lax.all_gather(w_out, "shard", axis=1, tiled=True),
        lax.all_gather(out_bias, "shard", axis=1, tiled=True),
        lax.all_gather(w_fc1, "shard", axis=1, tiled=True),
        lax.all_gather(fc1_bias, "shard", axis=1, tiled=True),
        lax.all_gather(w_fc2, "shard", axis=1, tiled=True),
    )

    def pair_source(key_local, value_local):
        return (
            lax.all_gather(key_local, "shard", axis=0, tiled=True),
            lax.all_gather(value_local, "shard", axis=0, tiled=True),
        )

    back_gains = regathered[0].astype(jnp.float32)

    def backward_step(sums, item):
        saved, kept_pair, d_output, seg_row = item
        (
            normed_one,
            unit_one,
            factor_one,
            queries,
            key_local,
            value_local,
            log_total,
            attn_mixed,
            unit_two,
            factor_two,
            normed_two,
            pre_act,
        ) = saved
        query_seg = lax.dynamic_slice_in_dim(seg_row, shard_index * row_count, row_count)
        key_back, value_back = pair_source(key_local, value_local)
        activated_f32, gelu_pull = jax.vjp(gelu_tanh, pre_act)
        activated = activated_f32.astype(jnp.bfloat16)
        d_out_f32 = d_output.astype(jnp.float32)
        g_fc2 = jnp.einsum("tf,td->fd", activated, d_output, preferred_element_type=jnp.float32)
        d_act = jnp.einsum("td,fd->tf", d_output, regathered[8], preferred_element_type=jnp.float32)
        d_pre = gelu_pull(d_act)[0].astype(jnp.bfloat16)
        g_fc1 = jnp.einsum("td,tf->df", normed_two, d_pre, preferred_element_type=jnp.float32)
        g_fc1_row = jnp.sum(d_pre.astype(jnp.float32), 0)
        d_norm_two = jnp.einsum(
            "tf,df->td", d_pre, regathered[6], preferred_element_type=jnp.float32
        )
        d_residual = d_out_f32 + norm_back(d_norm_two, unit_two, factor_two, back_gains[1])
        g_gain_two = jnp.sum(d_norm_two * unit_two, 0)
        g_bias_two = jnp.sum(d_norm_two, 0)
        d_branch = d_residual.astype(jnp.bfloat16)
        g_wout = jnp.einsum("td,te->de", attn_mixed, d_branch, preferred_element_type=jnp.float32)
        g_out_zero = jnp.sum(d_branch.astype(jnp.float32), 0)
        g_out_one = jnp.sum(d_out_f32, 0)
        d_mixed = jnp.einsum(
            "te,de->td", d_branch, regathered[4], preferred_element_type=jnp.float32
        )
        d_mixed = d_mixed.astype(jnp.bfloat16).reshape(row_count, HEADS, HEAD_DIM)
        d_queries, kv_term = attention_backward(
            queries, key_back, value_back, d_mixed, log_total, query_pos, query_seg, seg_row
        )
        kv_grad = lax.psum_scatter(
            kv_term.astype(jnp.bfloat16), "shard", scatter_dimension=0, tiled=True
        ).astype(jnp.float32)
        d_qkv = jnp.concatenate([d_queries.reshape(row_count, features), kv_grad], 1).astype(
            jnp.bfloat16
        )
        g_wqkv = jnp.einsum("td,tc->dc", normed_one, d_qkv, preferred_element_type=jnp.float32)
        d_qkv_f32 = d_qkv.astype(jnp.float32)
        g_qv_row = jnp.concatenate(
            [jnp.sum(d_qkv_f32[:, :features], 0), jnp.sum(d_qkv_f32[:, 2 * features :], 0)]
        )
        d_norm_one = jnp.einsum(
            "tc,dc->td", d_qkv, regathered[2], preferred_element_type=jnp.float32
        )
        d_tokens = d_residual + norm_back(d_norm_one, unit_one, factor_one, back_gains[0])
        g_gain_one = jnp.sum(d_norm_one * unit_one, 0)
        g_bias_one = jnp.sum(d_norm_one, 0)
        local_grads = (
            jnp.stack([g_gain_one, g_gain_two]),
            jnp.stack([g_bias_one, g_bias_two]),
            g_wqkv,
            g_qv_row[None],
            g_wout,
            jnp.stack([g_out_zero, g_out_one]),
            g_fc1,
            g_fc1_row[None],
            g_fc2,
        )
        new_sums = tuple((old + new for old, new in zip(sums, local_grads)))
        return (new_sums, d_tokens.astype(jnp.bfloat16))

    zero_sums = tuple((jnp.zeros(item.shape, jnp.float32) for item in regathered))
    grad_sums, d_inputs = lax.scan(
        backward_step, zero_sums, (saved_all, kept_all, cotangent, segments)
    )
    owned = (
        lax.psum_scatter(
            grad_sums[0].astype(jnp.bfloat16), "shard", scatter_dimension=1, tiled=True
        ).astype(jnp.float32),
        lax.psum_scatter(
            grad_sums[1].astype(jnp.bfloat16), "shard", scatter_dimension=1, tiled=True
        ).astype(jnp.float32),
        lax.psum_scatter(
            grad_sums[2].astype(jnp.bfloat16), "shard", scatter_dimension=1, tiled=True
        ).astype(jnp.float32),
        lax.psum_scatter(
            grad_sums[3].astype(jnp.bfloat16), "shard", scatter_dimension=1, tiled=True
        ).astype(jnp.float32),
        lax.psum_scatter(
            grad_sums[4].astype(jnp.bfloat16), "shard", scatter_dimension=1, tiled=True
        ).astype(jnp.float32),
        lax.psum_scatter(
            grad_sums[5].astype(jnp.bfloat16), "shard", scatter_dimension=1, tiled=True
        ).astype(jnp.float32),
        lax.psum_scatter(
            grad_sums[6].astype(jnp.bfloat16), "shard", scatter_dimension=1, tiled=True
        ).astype(jnp.float32),
        lax.psum_scatter(
            grad_sums[7].astype(jnp.bfloat16), "shard", scatter_dimension=1, tiled=True
        ).astype(jnp.float32),
        lax.psum_scatter(
            grad_sums[8].astype(jnp.bfloat16), "shard", scatter_dimension=1, tiled=True
        ).astype(jnp.float32),
    )
    summed = (
        lax.psum(owned[0].astype(jnp.bfloat16), "rep").astype(jnp.float32),
        lax.psum(owned[1].astype(jnp.bfloat16), "rep").astype(jnp.float32),
        lax.psum(owned[2].astype(jnp.bfloat16), "rep").astype(jnp.float32),
        lax.psum(owned[3].astype(jnp.bfloat16), "rep").astype(jnp.float32),
        lax.psum(owned[4].astype(jnp.bfloat16), "rep").astype(jnp.float32),
        lax.psum(owned[5].astype(jnp.bfloat16), "rep").astype(jnp.float32),
        lax.psum(owned[6].astype(jnp.bfloat16), "rep").astype(jnp.float32),
        lax.psum(owned[7].astype(jnp.bfloat16), "rep").astype(jnp.float32),
        lax.psum(owned[8].astype(jnp.bfloat16), "rep").astype(jnp.float32),
    )
    return (outputs, d_inputs) + tuple(summed)


HEAD_LANES = 2 * HEAD_DIM


def dot_nt(left, right):
    return lax.dot_general(left, right, (((1,), (1,)), ((), ())), preferred_element_type=jnp.float32)


def dot_nn(left, right):
    return lax.dot_general(left, right, (((1,), (0,)), ((), ())), preferred_element_type=jnp.float32)


def dot_tn(left, right):
    return lax.dot_general(left, right, (((0,), (0,)), ((), ())), preferred_element_type=jnp.float32)


def head_lane_masks(rows):
    lane = lax.broadcasted_iota(jnp.int32, (rows, HEAD_LANES), 1)
    limit = jnp.where(pl.program_id(0) == pl.num_programs(0) - 1, HEAD_DIM * (2 - HEADS % 2), HEAD_LANES)
    return (lane < HEAD_DIM), (lane >= HEAD_DIM) & (lane < limit)


def allowed_bias(low_ref, high_ref, rpos_ref, rseg_ref, cpos_ref, cseg_ref):
    half = rpos_ref.shape[0] // 2
    for ref, start, pieces in (
        (low_ref, 0, ((0, half), (2 * half, 3 * half))),
        (high_ref, half, ((0, half), (2 * half, 3 * half), (3 * half, 4 * half), (half, 2 * half))),
    ):
        rpos = rpos_ref[start : start + half, :]
        rseg = rseg_ref[start : start + half, :]
        at = 0
        for first, last in pieces:
            fits = (cpos_ref[:, first:last] <= rpos) & (cseg_ref[:, first:last] == rseg)
            ref[:, at : at + half] = jnp.where(fits, 0.0, -1e30)
            at += half


def gather_keys(own, other, half):
    low = jnp.concatenate([own[:half], other[:half]], 0)
    high = jnp.concatenate([own[:half], other, own[half:]], 0)
    return low, high


def attend_kernel(rpos, rseg, cpos, cseg, q_ref, ko_ref, kp_ref, vo_ref, vp_ref, out_ref, lse_ref, low_ref, high_ref):
    rows = q_ref.shape[0]
    half = rows // 2

    @pl.when(pl.program_id(0) == 0)
    def _():
        allowed_bias(low_ref, high_ref, rpos, rseg, cpos, cseg)

    first, second = head_lane_masks(rows)
    zero = jnp.zeros((), jnp.bfloat16)
    queries = q_ref[...]
    keys_own = jnp.where(first | second, ko_ref[...], zero)
    keys_other = jnp.where(first | second, kp_ref[...], zero)
    values_own, values_other = vo_ref[...], vp_ref[...]
    outs = [None, None]
    for head, lanes in enumerate((first, second)):
        query = jnp.where(lanes, queries, zero)
        v_own = jnp.where(lanes, values_own, zero)
        v_other = jnp.where(lanes, values_other, zero)
        key_parts = gather_keys(keys_own, keys_other, half)
        value_parts = gather_keys(v_own, v_other, half)
        for part, bias_ref in enumerate((low_ref, high_ref)):
            scores = dot_nt(query[part * half : (part + 1) * half], key_parts[part]) + bias_ref[...]
            top = jnp.max(scores, -1, keepdims=True)
            expo = jnp.exp(scores - top)
            total = jnp.sum(expo, -1, keepdims=True)
            mixed = dot_nn(expo.astype(jnp.bfloat16), value_parts[part]) / total
            outs[part] = mixed if outs[part] is None else outs[part] + mixed
            lse_ref[part * half : (part + 1) * half, head : head + 1] = top + jnp.log(total)
    out_ref[...] = jnp.concatenate(outs, 0).astype(jnp.bfloat16)


def attend_back_kernel(
    rpos, rseg, cpos, cseg, q_ref, ko_ref, kp_ref, vo_ref, vp_ref, do_ref, lse_ref,
    dq_ref, dko_ref, dkp_ref, dvo_ref, dvp_ref, low_ref, high_ref,
):
    rows = q_ref.shape[0]
    half = rows // 2

    @pl.when(pl.program_id(0) == 0)
    def _():
        allowed_bias(low_ref, high_ref, rpos, rseg, cpos, cseg)

    first, second = head_lane_masks(rows)
    zero = jnp.zeros((), jnp.bfloat16)
    queries, grads = q_ref[...], do_ref[...]
    both = first | second
    keys_own = jnp.where(both, ko_ref[...], zero)
    keys_other = jnp.where(both, kp_ref[...], zero)
    values_own = jnp.where(both, vo_ref[...], zero)
    values_other = jnp.where(both, vp_ref[...], zero)
    key_sums, value_sums = [None] * 4, [None] * 4
    query_sums = [None, None]

    def add(sums, at, new):
        sums[at] = new if sums[at] is None else sums[at] + new

    order = ((0, 2), (0, 2, 3, 1))
    for head, lanes in enumerate((first, second)):
        query = jnp.where(lanes, queries, zero)
        grad = jnp.where(lanes, grads, zero)
        key_own = jnp.where(lanes, keys_own, zero)
        key_other = jnp.where(lanes, keys_other, zero)
        key_parts = gather_keys(key_own, key_other, half)
        value_parts = gather_keys(values_own, values_other, half)
        for part, bias_ref in enumerate((low_ref, high_ref)):
            span = slice(part * half, (part + 1) * half)
            scores = dot_nt(query[span], key_parts[part]) + bias_ref[...]
            probs = jnp.exp(scores - lse_ref[span, head : head + 1])
            d_probs = dot_nt(grad[span], value_parts[part])
            weighed = probs * d_probs
            delta = jnp.sum(weighed, -1, keepdims=True)
            d_scores = (weighed - probs * delta).astype(jnp.bfloat16)
            add(query_sums, part, dot_nn(d_scores, key_parts[part]))
            d_key = dot_tn(d_scores, query[span])
            d_value = dot_tn(probs.astype(jnp.bfloat16), grad[span])
            for at, block in enumerate(order[part]):
                add(key_sums, block, d_key[at * half : (at + 1) * half])
                add(value_sums, block, d_value[at * half : (at + 1) * half])
    dq_ref[...] = jnp.concatenate(query_sums, 0) * HEAD_DIM ** (-0.5)
    dko_ref[...] = jnp.concatenate(key_sums[:2], 0)
    dkp_ref[...] = jnp.concatenate(key_sums[2:], 0).astype(jnp.bfloat16)
    dvo_ref[...] = jnp.concatenate(value_sums[:2], 0)
    dvp_ref[...] = jnp.concatenate(value_sums[2:], 0).astype(jnp.bfloat16)


def attention_specs(rows, extra):
    whole = lambda shape: pl.BlockSpec(shape, lambda j: (0, 0))
    block = pl.BlockSpec((rows, HEAD_LANES), lambda j: (0, j))
    ins = [whole((rows, 1)), whole((rows, 1)), whole((1, 2 * rows)), whole((1, 2 * rows))]
    return ins, block


def attend(marks, queries, own_k, other_k, own_v, other_v):
    rows, features = queries.shape
    pairs = pl.cdiv(features, HEAD_LANES)
    ins, block = attention_specs(rows, 0)
    lse = pl.BlockSpec((None, rows, 2), lambda j: (j, 0, 0))
    return pl.pallas_call(
        attend_kernel,
        grid=(pairs,),
        in_specs=ins + [block] * 5,
        out_specs=[block, lse],
        out_shape=[
            jax.ShapeDtypeStruct((rows, features), jnp.bfloat16),
            jax.ShapeDtypeStruct((pairs, rows, 2), jnp.float32),
        ],
        scratch_shapes=[pltpu.VMEM((rows // 2, rows), jnp.float32), pltpu.VMEM((rows // 2, 2 * rows), jnp.float32)],
        cost_estimate=pl.CostEstimate(flops=8 * rows * rows * features, bytes_accessed=12 * rows * features, transcendentals=0),
        name="attend",
    )(*marks, queries, own_k, other_k, own_v, other_v)


def attend_back(marks, queries, own_k, other_k, own_v, other_v, grads, lse_rows):
    rows, features = queries.shape
    pairs = pl.cdiv(features, HEAD_LANES)
    ins, block = attention_specs(rows, 0)
    lse = pl.BlockSpec((None, rows, 2), lambda j: (j, 0, 0))
    wide = jax.ShapeDtypeStruct((rows, features), jnp.float32)
    slim = jax.ShapeDtypeStruct((rows, features), jnp.bfloat16)
    return pl.pallas_call(
        attend_back_kernel,
        grid=(pairs,),
        in_specs=ins + [block] * 6 + [lse],
        out_specs=[block] * 5,
        out_shape=[wide, wide, slim, wide, slim],
        scratch_shapes=[pltpu.VMEM((rows // 2, rows), jnp.float32), pltpu.VMEM((rows // 2, 2 * rows), jnp.float32)],
        cost_estimate=pl.CostEstimate(flops=20 * rows * rows * features, bytes_accessed=30 * rows * features, transcendentals=0),
        name="attend_back",
    )(*marks, queries, own_k, other_k, own_v, other_v, grads, lse_rows)


def trade_lists(shard_count, rep_count):
    first, second = [], []
    for shard in range(shard_count):
        for rep in range(rep_count):
            core = rep % 2
            outer = (shard >= shard_count // 2) * 1
            target_core = 0 if shard in (0, shard_count - 1) else 1
            for moves, local in ((first, outer), (second, 1 - outer)):
                target = (2 * core + local) * rep_count + (rep - core + target_core)
                moves.append((shard * rep_count + rep, target))
    return first, second


BOTH = ("shard", "rep")


def to_sequence(blocks, moves, shard_index):
    upper = shard_index >= 2
    one = lax.ppermute(jnp.where(upper, blocks[1], blocks[0]), BOTH, moves[0])
    two = lax.ppermute(jnp.where(upper, blocks[0], blocks[1]), BOTH, moves[1])
    even = shard_index % 2 == 0
    return jnp.concatenate([jnp.where(even, one, two), jnp.where(even, two, one)], 0)


def from_sequence(rows, moves, shard_index):
    half = rows.shape[0] // 2
    low, high = rows[:half], rows[half:]
    even = shard_index % 2 == 0
    back = [[(b, a) for a, b in move] for move in moves]
    one = lax.ppermute(jnp.where(even, low, high), BOTH, back[0])
    two = lax.ppermute(jnp.where(even, high, low), BOTH, back[1])
    upper = shard_index >= 2
    return jnp.stack([jnp.where(upper, two, one), jnp.where(upper, one, two)])


def swap_core(array, rep_count):
    return lax.ppermute(array, "rep", [(r, r ^ 1) for r in range(rep_count)])


def gather_weights(w_qkv, w_out, w_fc1, w_fc2, smalls):
    features = w_qkv.shape[0]
    rep = lax.axis_index("rep")
    part = w_out.shape[1]
    side = jnp.concatenate([w_qkv, w_out, w_fc1], 1)
    piece = lax.dynamic_slice(side, (0, rep * part), (features, part)).T
    half = part // 2
    tail = lax.dynamic_slice(w_fc2, ((rep // 2) * features, (rep % 2) * half), (features, half)).T
    small = jnp.zeros((8, features), jnp.bfloat16).at[:3].set(smalls)
    head = lax.all_gather(jnp.concatenate([piece, small], 0), BOTH, axis=0).reshape(4, 8, part + 8, features)
    rest = lax.all_gather(tail, BOTH, axis=0).reshape(4, 4, part, features)
    qkv = head[:, 0:3, :part].reshape(3 * features, features)
    out = head[:, 3, :part].reshape(features, features)
    fc1 = head[:, 4:8, :part].reshape(4 * features, features)
    fc2 = rest.transpose(1, 0, 2, 3).reshape(4, features, features)
    return qkv, out, fc1, fc2, head[:, 0, part : part + 3]


def reduce_rows(grads):
    rows = lax.psum_scatter(grads.astype(jnp.bfloat16), "rep", scatter_dimension=1, tiled=True)
    rows = lax.psum_scatter(rows, "shard", scatter_dimension=0, tiled=True)
    return lax.all_gather(rows, "rep", axis=1, tiled=True)[0]


def shards_by_sequence(
    inputs, segments, cotangent, ln_gain, ln_bias, w_qkv, qv_bias, w_out, out_bias, w_fc1, fc1_bias, w_fc2
):
    features = inputs.shape[2]
    block = inputs.shape[1]
    rep_count = lax.axis_size("rep")
    moves = trade_lists(4, rep_count)
    shard_index = lax.axis_index("shard")
    core = lax.axis_index("rep") % 2
    f32 = jnp.float32
    smalls = jnp.concatenate(
        [ln_gain.reshape(-1), ln_bias.reshape(-1), qv_bias.reshape(-1), out_bias.reshape(-1), fc1_bias.reshape(-1)]
    ).reshape(3, features)
    wq, wo, w1, w2, small_rows = gather_weights(w_qkv, w_out, w_fc1, w_fc2, smalls)
    small_rows = small_rows.reshape(4, 3 * features).astype(f32)
    part = features // 4
    gains = [small_rows[:, 0:part].reshape(-1), small_rows[:, part : 2 * part].reshape(-1)]
    biases = [small_rows[:, 2 * part : 3 * part].reshape(-1), small_rows[:, 3 * part : 4 * part].reshape(-1)]
    qv_row = small_rows[:, 4 * part : 6 * part].reshape(-1)
    out_rows = [small_rows[:, 6 * part : 7 * part].reshape(-1), small_rows[:, 7 * part : 8 * part].reshape(-1)]
    fc1_row = small_rows[:, 8 * part :].reshape(-1)

    tokens = to_sequence(inputs, moves, shard_index).astype(f32)
    d_output = to_sequence(cotangent, moves, shard_index)
    partner_segments = swap_core(segments, rep_count)
    mine_has = (shard_index // 2) == core
    local = shard_index % 2
    seg_row = jnp.where(
        mine_has,
        lax.dynamic_index_in_dim(segments, local, 0, keepdims=False),
        lax.dynamic_index_in_dim(partner_segments, local, 0, keepdims=False),
    )
    low_own = jnp.where(core == 0, 0, 1)
    high_own = jnp.where(core == 0, 3, 2)
    spots = jnp.stack([low_own, high_own, 1 - low_own, 5 - high_own])
    pos = (spots[:, None] * block + jnp.arange(block, dtype=jnp.int32)[None]).reshape(-1)
    segs = seg_row.reshape(4, block)
    seg = jnp.concatenate([lax.dynamic_index_in_dim(segs, spots[i], 0, keepdims=False) for i in range(4)])
    rows = 2 * block
    marks = (pos[:rows, None], seg[:rows, None], pos[None], seg[None])

    normed_f32, unit_one, factor_one = layer_norm(tokens, gains[0], biases[0])
    normed_one = normed_f32.astype(jnp.bfloat16)
    own_k = dot_nt(normed_one, wq[features : 2 * features]).astype(jnp.bfloat16)
    own_v = (dot_nt(normed_one, wq[2 * features :]) + qv_row[features:]).astype(jnp.bfloat16)
    other_k, other_v = swap_core(own_k, rep_count), swap_core(own_v, rep_count)
    queries = (dot_nt(normed_one, wq[:features]) + qv_row[:features]).astype(jnp.bfloat16)
    queries = queries * jnp.asarray(HEAD_DIM ** (-0.5), jnp.bfloat16)
    attn_mixed, lse_rows = attend(marks, queries, own_k, other_k, own_v, other_v)
    residual = tokens + (dot_nt(attn_mixed, wo) + out_rows[0])
    normed_f32, unit_two, factor_two = layer_norm(residual, gains[1], biases[1])
    normed_two = normed_f32.astype(jnp.bfloat16)
    pre_act = dot_nt(normed_two, w1) + fc1_row
    activated_f32, gelu_pull = jax.vjp(gelu_tanh, pre_act)
    activated = activated_f32.astype(jnp.bfloat16)
    output = residual + out_rows[1]
    for i in range(4):
        output = output + dot_nt(activated[:, i * features : (i + 1) * features], w2[i])
    outputs = from_sequence(output.astype(jnp.bfloat16), moves, shard_index)

    d_out_f32 = d_output.astype(f32)
    d_act = jnp.concatenate([dot_nn(d_output, w2[i]) for i in range(4)], 1)
    d_pre = gelu_pull(d_act)[0].astype(jnp.bfloat16)
    g_fc1 = dot_tn(d_pre, normed_two).reshape(4, features, features)
    g_fc2 = jnp.stack(
        [dot_tn(d_output, activated[:, i * features : (i + 1) * features]).reshape(4, part, features) for i in range(4)], 1
    ).reshape(4, features, features)
    fc_owned = reduce_rows(jnp.concatenate([g_fc1, g_fc2], 1))
    g_fc1_row = jnp.sum(d_pre.astype(f32), 0)
    d_norm_two = dot_nn(d_pre, w1)
    d_residual = d_out_f32 + norm_back(d_norm_two, unit_two, factor_two, gains[1])
    g_gain_two = jnp.sum(d_norm_two * unit_two, 0)
    g_bias_two = jnp.sum(d_norm_two, 0)
    d_branch = d_residual.astype(jnp.bfloat16)
    d_mixed = dot_nn(d_branch, wo).astype(jnp.bfloat16)
    d_q, dk_own, dk_other, dv_own, dv_other = attend_back(
        marks, queries, own_k, other_k, own_v, other_v, d_mixed, lse_rows
    )
    d_q = d_q.astype(jnp.bfloat16)
    d_k = (dk_own + swap_core(dk_other, rep_count).astype(f32)).astype(jnp.bfloat16)
    d_v = (dv_own + swap_core(dv_other, rep_count).astype(f32)).astype(jnp.bfloat16)
    g_wout = dot_tn(d_branch, attn_mixed).reshape(4, part, features)
    g_wqkv = jnp.concatenate([dot_tn(d, normed_one) for d in (d_q, d_k, d_v)], 0).reshape(4, 3 * part, features)
    d_norm_one = (
        dot_nn(d_q, wq[:features]) + dot_nn(d_k, wq[features : 2 * features]) + dot_nn(d_v, wq[2 * features :])
    )
    d_tokens = d_residual + norm_back(d_norm_one, unit_one, factor_one, gains[0])
    d_inputs = from_sequence(d_tokens.astype(jnp.bfloat16), moves, shard_index)
    g_qv_row = jnp.concatenate([jnp.sum(d_q.astype(f32), 0), jnp.sum(d_v.astype(f32), 0)])
    side_grads = [
        jnp.sum(d_norm_one * unit_one, 0),
        g_gain_two,
        jnp.sum(d_norm_one, 0),
        g_bias_two,
        g_qv_row,
        jnp.sum(d_branch.astype(f32), 0),
        jnp.sum(d_out_f32, 0),
        g_fc1_row,
    ]
    small_grads = jnp.concatenate([item.reshape(4, -1) for item in side_grads], 1)
    small_owned = lax.psum(lax.psum_scatter(small_grads, "shard", scatter_dimension=0, tiled=True), "rep")[0]
    attn_owned = reduce_rows(jnp.concatenate([g_wqkv, g_wout], 1))

    def back(rows_in):
        return rows_in.T.astype(f32)

    g_fc2_owned = fc_owned[features:].reshape(4, part, features).transpose(0, 2, 1).reshape(4 * features, part)
    return (
        outputs,
        d_inputs,
        small_owned[: 2 * part].reshape(2, part),
        small_owned[2 * part : 4 * part].reshape(2, part),
        back(attn_owned[: 3 * part]),
        small_owned[4 * part : 6 * part].reshape(1, 2 * part),
        back(attn_owned[3 * part :]),
        small_owned[6 * part : 8 * part].reshape(2, part),
        back(fc_owned[:features]),
        small_owned[8 * part :].reshape(1, 4 * part),
        g_fc2_owned.astype(f32),
    )


def solution(mesh):
    shard_count, rep_count = mesh.shape["shard"], mesh.shape["rep"]
    by_sequence = shard_count == 4 and rep_count == 8
    placed = (
        P("rep", "shard", None),
        P("rep", None),
        P("rep", "shard", None),
        P(None, "shard"),
        P(None, "shard"),
        P(None, "shard"),
        P(None, "shard"),
        P(None, "shard"),
        P(None, "shard"),
        P(None, "shard"),
        P(None, "shard"),
        P(None, "shard"),
    )
    return jax.shard_map(
        shards_by_sequence if by_sequence else shards,
        mesh=mesh,
        in_specs=placed,
        out_specs=(
            P("rep", "shard", None),
            P("rep", "shard", None),
            P(None, "shard"),
            P(None, "shard"),
            P(None, "shard"),
            P(None, "shard"),
            P(None, "shard"),
            P(None, "shard"),
            P(None, "shard"),
            P(None, "shard"),
            P(None, "shard"),
        ),
        check_vma=False,
    )
```
